8 devices in a mesh: stage: 2 (over z, y), expert: 4 (over x, core).
Axes of the slice: x: 2, y: 2, z: 1, core: 2. Of those that a mesh axis runs over, the one named last changes fastest.
Arguments:
- w_gate: bfloat16 [12, 16, 1024, 512], P('stage', 'expert')
- w_up: bfloat16 [12, 16, 1024, 512], P('stage', 'expert')
- w_down: bfloat16 [12, 16, 512, 1024], P('stage', 'expert')
- x: bfloat16 [2048, 1024], P(('stage', 'expert'))
- expert_ids: int32 [12, 2048, 8], P(None, ('stage', 'expert'))
- gates: float32 [12, 2048, 8], P(None, ('stage', 'expert'))
Outputs:
- output 1: bfloat16 [12, 16, 1024, 1024], P(None, ('stage', 'expert'))
- output 2: bfloat16 [12, 16, 512, 1024], P(None, ('stage', 'expert'))
- output 3: float32 [12, 2048, 1024], P(None, ('stage', 'expert'))
All inputs are finite; a program needn't handle non-finite values.
Results may differ from the reference program's by a relative error of at most 0.00555969.
Values are sent between devices in bfloat16 or wider.
A program may use at most 1 GiB of HBM per device.

```python
import jax
import jax.numpy as jnp
from jax import lax

D = 1024
FF = 512
TOP = 8
LAYERS = 12
EXPERTS = 16
DEVICES = 8
TOK_DEV = 256

TOKENS = DEVICES * TOK_DEV
CAPACITY = 3 * TOK_DEV * TOP // (2 * EXPERTS)
NORM_EPS = 1e-6


def draw_routes(key):
    mean_load = TOK_DEV * TOP // EXPERTS
    half_load = mean_load // 2
    blocks = LAYERS * DEVICES
    key_shift, key_expert, key_token = jax.random.split(key, 3)
    shifts = jax.random.randint(key_shift, (blocks, EXPERTS // 2), 0, half_load + 1)
    shifts = shifts.at[:, 0].set(half_load)
    counts = jnp.stack([mean_load + shifts, mean_load - shifts], axis=-1).reshape(blocks, EXPERTS)
    run_ends = jnp.cumsum(counts, axis=-1)
    entry = jnp.arange(TOK_DEV * TOP)
    virtual = jnp.sum((entry[None, :, None] >= run_ends[:, None, :]).astype(jnp.int32), axis=-1)
    expert_perm = jax.vmap(lambda sub_key: jax.random.permutation(sub_key, EXPERTS))(jax.random.split(key_expert, blocks))
    labels = jax.vmap(lambda table, index: table[index])(expert_perm, virtual)
    labels = jnp.transpose(labels.reshape(blocks, TOP, TOK_DEV), (0, 2, 1))
    token_perm = jax.vmap(lambda sub_key: jax.random.permutation(sub_key, TOK_DEV))(jax.random.split(key_token, blocks))
    routed = jax.vmap(lambda table, index: table[index])(labels, token_perm)
    return routed.reshape(LAYERS, TOKENS, TOP).astype(jnp.int32)


def setup_inputs(seed: int = 0) -> dict:
    key = jax.random.key(seed)
    key_gate, key_up, key_down, key_x, key_mix, key_route = jax.random.split(key, 6)
    w_gate = (jax.random.normal(key_gate, (LAYERS, EXPERTS, D, FF), jnp.float32) * D ** -0.5).astype(jnp.bfloat16)
    w_up = (jax.random.normal(key_up, (LAYERS, EXPERTS, D, FF), jnp.float32) * D ** -0.5).astype(jnp.bfloat16)
    w_down = (jax.random.normal(key_down, (LAYERS, EXPERTS, FF, D), jnp.float32) * FF ** -0.5).astype(jnp.bfloat16)
    x = jax.random.normal(key_x, (TOKENS, D), jnp.float32).astype(jnp.bfloat16)
    gates = jax.nn.softmax(jax.random.normal(key_mix, (LAYERS, TOKENS, TOP), jnp.float32), axis=-1)
    expert_ids = draw_routes(key_route)
    return {"w_gate": w_gate, "w_up": w_up, "w_down": w_down, "x": x, "expert_ids": expert_ids, "gates": gates}


def expert_layer(hidden, layer_in):
    layer_w13, layer_down, layer_ids, layer_mix = layer_in
    normed = (hidden * lax.rsqrt(jnp.mean(hidden * hidden, axis=-1, keepdims=True) + NORM_EPS)).astype(jnp.bfloat16)
    flat_ids = layer_ids.reshape(-1)
    onehot = (flat_ids[:, None] == jnp.arange(EXPERTS)[None, :]).astype(jnp.int32)
    pair_rank = jnp.sum(onehot * jnp.cumsum(onehot, axis=0), axis=-1) - 1
    rows_per_expert = DEVICES * CAPACITY
    slot_pos = flat_ids * rows_per_expert + pair_rank
    pair_tok = jnp.arange(TOKENS * TOP) // TOP
    buffer = jnp.zeros((EXPERTS * rows_per_expert, D), jnp.bfloat16).at[slot_pos].set(normed[pair_tok])
    buffer = buffer.reshape(EXPERTS, rows_per_expert, D).astype(jnp.float32)
    projected = jnp.einsum("erd,edg->erg", buffer, layer_w13.astype(jnp.float32))
    activated = (jax.nn.silu(projected[..., :FF]) * projected[..., FF:]).astype(jnp.bfloat16)
    expert_out = jnp.einsum("erf,efd->erd", activated.astype(jnp.float32), layer_down.astype(jnp.float32)).astype(jnp.bfloat16)
    picked = expert_out.reshape(EXPERTS * rows_per_expert, D)[slot_pos].astype(jnp.float32).reshape(TOKENS, TOP, D)
    new_hidden = hidden + jnp.sum(layer_mix[..., None] * picked, axis=1)
    return new_hidden, new_hidden


def reference(w_gate, w_up, w_down, x, expert_ids, gates):
    w13 = jnp.concatenate([w_gate, w_up], axis=-1)
    _, hiddens = lax.scan(expert_layer, x.astype(jnp.float32), (w13, w_down, expert_ids, gates))
    return w13, w_down, hiddens
```

```python
import functools

import jax
import jax.numpy as jnp
from jax import lax
from jax.experimental import pallas as pl
from jax.experimental.pallas import tpu as pltpu
from jax.sharding import PartitionSpec as P

NORM_EPS = 1e-6
FLAT = ("stage", "expert")
MESH = pl.DeviceIdType.MESH
PART_A = 4


def moe_kernel(gate_hbm, up_hbm, down_hbm, x_vmem, mix_vmem, w13_hbm, wd_hbm, hid_hbm, w13_buf, wd_buf, u_buf, p_buf, r_buf, h_buf, g_buf, w_send, w_recv, load_sem, push_send, push_recv, u_send, u_recv, p_send, p_recv, g_send, g_recv, out_sem, credit):
    lay_stage, exp_grp = gate_hbm.shape[0], gate_hbm.shape[1]
    n_layers = hid_hbm.shape[0]
    ff = gate_hbm.shape[3]
    n_experts = exp_grp * 4
    sy = lax.axis_index("stage")
    sg = lax.axis_index("expert")
    sx, sc = sg // 2, sg % 2
    dst_y, dst_x = sx, sc
    partner = (sy, 2 * sx + 1 - sc)
    first_expert = 8 * sy + 4 * sx

    def peer(j):
        return ((sy + j // 2) % 2, 2 * ((sx + j % 2) % 2) + sc)

    def weight_parts(k, dst_core, j):
        layer = sy * lay_stage + k
        src_e = 2 * dst_core + j
        return (
            (gate_hbm.at[k, src_e], w13_hbm.at[layer, j, :, pl.ds(0, ff)]),
            (up_hbm.at[k, src_e], w13_hbm.at[layer, j, :, pl.ds(ff, ff)]),
            (down_hbm.at[k, src_e], wd_hbm.at[layer, j]),
        )

    def is_self(dst_core):
        return (dst_y == sy) & (2 * dst_x + dst_core == sg)

    def weight_remote(k, dst_core, j, i):
        src, dst = weight_parts(k, dst_core, j)[i]
        return pltpu.make_async_remote_copy(src, dst, w_send.at[k, dst_core, j, i], w_recv.at[sy * lay_stage + k, j, i], device_id=(dst_y, 2 * dst_x + dst_core), device_id_type=MESH)

    def weight_local(k, dst_core, j, i):
        src, dst = weight_parts(k, dst_core, j)[i]
        return pltpu.make_async_copy(src, dst, w_recv.at[sy * lay_stage + k, j, i])

    def send_weights(k, part_lo, part_hi):
        for idx in range(part_lo, part_hi):
            i, dst_core, j = idx % 3, (idx // 3) % 2, idx // 6

            @pl.when(is_self(dst_core))
            def _():
                weight_local(k, dst_core, j, i).start()

            @pl.when(jnp.logical_not(is_self(dst_core)))
            def _():
                weight_remote(k, dst_core, j, i).start()

    def landed(layer, j, i):
        dst = (w13_hbm.at[layer, j, :, pl.ds(0, ff)], w13_hbm.at[layer, j, :, pl.ds(ff, ff)], wd_hbm.at[layer, j])[i]
        src = (gate_hbm.at[0, 0], up_hbm.at[0, 0], down_hbm.at[0, 0])[i]
        return pltpu.make_async_copy(src, dst, w_recv.at[layer, j, i])

    def load_parts(layer, j):
        slot = layer % 2
        return (
            (w13_hbm.at[layer, j], w13_buf.at[slot, 2 * sc + j]),
            (wd_hbm.at[layer, j], wd_buf.at[slot, 2 * sc + j]),
        )

    def load_local(layer, j, i):
        src, dst = load_parts(layer, j)[i]
        return pltpu.make_async_copy(src, dst, load_sem.at[layer % 2, j, i])

    def load_push(layer, j, i):
        src, dst = load_parts(layer, j)[i]
        return pltpu.make_async_remote_copy(src, dst, push_send.at[layer % 2, j, i], push_recv.at[layer % 2, j, i], device_id=partner, device_id_type=MESH)

    def start_load(layer):
        @pl.when(layer >= 2)
        def _():
            pl.semaphore_wait(credit, 1)

        for j in range(2):
            for i in range(3):
                landed(layer, j, i).wait()
            for i in range(2):
                load_local(layer, j, i).start()
                load_push(layer, j, i).start()

    def finish_load(layer):
        for j in range(2):
            for i in range(2):
                load_local(layer, j, i).wait()
                load_push(layer, j, i).wait()

    def u_copy(j):
        return pltpu.make_async_remote_copy(u_buf.at[0], u_buf.at[j], u_send.at[j], u_recv.at[j], device_id=peer(j), device_id_type=MESH)

    def p_copy(j):
        return pltpu.make_async_remote_copy(p_buf.at[j], r_buf.at[j], p_send.at[j], p_recv.at[j], device_id=peer(j), device_id_type=MESH)

    def g_copy(j):
        return pltpu.make_async_remote_copy(mix_vmem, g_buf.at[j], g_send.at[j], g_recv.at[j], device_id=peer(j), device_id_type=MESH)

    def out_copy(layer):
        return pltpu.make_async_copy(h_buf.at[(layer + 1) % 2], hid_hbm.at[layer], out_sem.at[(layer + 1) % 2])

    for j in (1, 2, 3):
        g_copy(j).start()
    send_weights(0, 0, 12)
    h_buf[0] = x_vmem[...].astype(jnp.float32)
    g_buf[0] = mix_vmem[...]
    for j in (1, 2, 3):
        g_copy(j).wait()

    lane = lax.broadcasted_iota(jnp.int32, g_buf.shape[1:], 1)

    @pl.loop(0, n_layers)
    def _(layer):
        slot = layer % 2
        h = h_buf[slot]
        u_buf[0] = (h * lax.rsqrt(jnp.mean(h * h, axis=-1, keepdims=True) + NORM_EPS)).astype(jnp.bfloat16)
        for j in (1, 2, 3):
            u_copy(j).start()

        @pl.when(layer < lay_stage - 1)
        def _():
            send_weights(layer + 1, 0, PART_A)

        @pl.when(layer < lay_stage)
        def _():
            start_load(layer)

        finish_load(layer)

        @pl.loop(0, 4)
        def _(b):
            @pl.when(b > 0)
            def _():
                u_copy(b).wait()

            p_buf[b] = jnp.zeros(p_buf.shape[1:], jnp.float32)

            @pl.loop(0, exp_grp)
            def _(e):
                z = jnp.dot(u_buf[b], w13_buf[slot, e], preferred_element_type=jnp.float32)
                a = (jax.nn.silu(z[:, :ff]) * z[:, ff:]).astype(jnp.bfloat16)
                o = jnp.dot(a, wd_buf[slot, e], preferred_element_type=jnp.float32).astype(jnp.bfloat16).astype(jnp.float32)
                column = layer * n_experts + first_expert + e
                mix = jnp.sum(jnp.where(lane == column, g_buf[b], 0.0), axis=-1, keepdims=True)
                p_buf[b] = p_buf[b] + jnp.where(mix > 0.0, mix * o, 0.0)

            @pl.when(b > 0)
            def _():
                p_copy(b).start()

        @pl.when(layer < n_layers - 2)
        def _():
            pl.semaphore_signal(credit, 1, device_id=partner, device_id_type=MESH)

        @pl.when(layer < lay_stage - 1)
        def _():
            send_weights(layer + 1, PART_A, 12)

        @pl.when((layer >= lay_stage - 1) & (layer < n_layers - 1))
        def _():
            start_load(layer + 1)

        @pl.when(layer >= 2)
        def _():
            out_copy(layer - 2).wait()

        for j in (1, 2, 3):
            p_copy(j).wait()
        h_buf[1 - slot] = h_buf[slot] + (p_buf[0] + r_buf[1] + r_buf[2] + r_buf[3])
        out_copy(layer).start()

    out_copy(n_layers - 2).wait()
    out_copy(n_layers - 1).wait()

    @pl.loop(0, lay_stage)
    def _(k):
        for idx in range(12):
            i, dst_core, j = idx % 3, (idx // 3) % 2, idx // 6

            @pl.when(jnp.logical_not(is_self(dst_core)))
            def _():
                weight_remote(k, dst_core, j, i).wait_send()


def solution(mesh):
    n_stage = mesh.shape["stage"]
    n_group = mesh.shape["expert"]

    def per_device(gate_loc, up_loc, down_loc, x_loc, ids_loc, mix_loc):
        lay_stage, exp_grp, width, ff = gate_loc.shape
        n_layers, tok = ids_loc.shape[0], ids_loc.shape[1]
        n_experts = exp_grp * n_group
        exp_dev = exp_grp // n_stage
        onehot = ids_loc[..., None] == jnp.arange(n_experts, dtype=jnp.int32)
        dense = jnp.sum(jnp.where(onehot, mix_loc[..., None], 0.0), axis=2)
        dense = jnp.transpose(dense, (1, 0, 2)).reshape(tok, n_layers * n_experts)
        lanes = -(-dense.shape[1] // 128) * 128
        dense = jnp.pad(dense, ((0, 0), (0, lanes - dense.shape[1])))
        any_spec = pl.BlockSpec(memory_space=pl.ANY)
        vmem_spec = pl.BlockSpec(memory_space=pltpu.VMEM)
        dma = pltpu.SemaphoreType.DMA
        return pl.pallas_call(
            moe_kernel,
            out_shape=(
                jax.ShapeDtypeStruct((n_layers, exp_dev, width, 2 * ff), jnp.bfloat16),
                jax.ShapeDtypeStruct((n_layers, exp_dev, ff, width), jnp.bfloat16),
                jax.ShapeDtypeStruct((n_layers, tok, width), jnp.float32),
            ),
            in_specs=[any_spec, any_spec, any_spec, vmem_spec, vmem_spec],
            out_specs=(any_spec, any_spec, any_spec),
            scratch_shapes=[
                pltpu.VMEM((2, exp_grp, width, 2 * ff), jnp.bfloat16),
                pltpu.VMEM((2, exp_grp, ff, width), jnp.bfloat16),
                pltpu.VMEM((4, tok, width), jnp.bfloat16),
                pltpu.VMEM((4, tok, width), jnp.float32),
                pltpu.VMEM((4, tok, width), jnp.float32),
                pltpu.VMEM((2, tok, width), jnp.float32),
                pltpu.VMEM((4, tok, lanes), jnp.float32),
                dma((lay_stage, 2, 2, 3)),
                dma((n_layers, 2, 3)),
                dma((2, 2, 2)),
                dma((2, 2, 2)),
                dma((2, 2, 2)),
                dma((4,)),
                dma((4,)),
                dma((4,)),
                dma((4,)),
                dma((4,)),
                dma((4,)),
                dma((2,)),
                pltpu.SemaphoreType.REGULAR,
            ],
            compiler_params=pltpu.CompilerParams(has_side_effects=True, vmem_limit_bytes=60 * 1024 * 1024),
        )(gate_loc, up_loc, down_loc, x_loc, dense)

    weight_spec = P("stage", "expert")
    token_spec = P(None, FLAT)
    return jax.shard_map(per_device, mesh=mesh, in_specs=(weight_spec, weight_spec, weight_spec, P(FLAT), token_spec, token_spec), out_specs=(token_spec, token_spec, token_spec), check_vma=False)
```

```python
import functools

import jax
import jax.numpy as jnp
from jax import lax
from jax.experimental import pallas as pl
from jax.experimental.pallas import tpu as pltpu
from jax.sharding import PartitionSpec as P

NORM_EPS = 1e-6
FLAT = ("stage", "expert")
MESH = pl.DeviceIdType.MESH
PART_A = 2
QUARTERS = 2


def moe_kernel(gate_hbm, up_hbm, down_hbm, x_vmem, mix_vmem, w13_hbm, wd_hbm, hid_hbm, w13_buf, wd_buf, u_buf, p_buf, r_buf, h_buf, g_buf, b13_buf, bd_buf, w_send, w_recv, load_sem, push_send, push_recv, u_send, u_recv, p_send, p_recv, g_send, g_recv, out_sem, credit):
    lay_stage, exp_grp = gate_hbm.shape[0], gate_hbm.shape[1]
    n_layers = hid_hbm.shape[0]
    ff = gate_hbm.shape[3]
    n_experts = exp_grp * 4
    sy = lax.axis_index("stage")
    sg = lax.axis_index("expert")
    sx, sc = sg // 2, sg % 2
    dst_y, dst_x = sx, sc
    partner = (sy, 2 * sx + 1 - sc)
    first_expert = 8 * sy + 4 * sx

    half = u_buf.shape[1] // 2
    quarter = half // QUARTERS

    def neighbour(axis):
        return ((sy, 2 * (1 - sx) + sc), (1 - sy, sg))[axis]

    def rows(h):
        return pl.ds(h * half, half)

    def part(h, q):
        return pl.ds(h * half + q * quarter, quarter)

    def weight_parts(k, dst_core, j):
        layer = sy * lay_stage + k
        src_e = 2 * dst_core + j
        return (
            (gate_hbm.at[k, src_e], w13_hbm.at[layer, j, :, pl.ds(0, ff)]),
            (up_hbm.at[k, src_e], w13_hbm.at[layer, j, :, pl.ds(ff, ff)]),
            (down_hbm.at[k, src_e], wd_hbm.at[layer, j]),
        )

    def is_self(dst_core):
        return (dst_y == sy) & (2 * dst_x + dst_core == sg)

    def weight_remote(k, dst_core, j, i):
        src, dst = weight_parts(k, dst_core, j)[i]
        return pltpu.make_async_remote_copy(src, dst, w_send.at[k, dst_core, j, i], w_recv.at[sy * lay_stage + k, j, i], device_id=(dst_y, 2 * dst_x + dst_core), device_id_type=MESH)

    def bounce(j, i):
        return (b13_buf.at[j, :, pl.ds(0, ff)], b13_buf.at[j, :, pl.ds(ff, ff)], bd_buf.at[j])[i]

    def weight_read(k, dst_core, j, i):
        return pltpu.make_async_copy(weight_parts(k, dst_core, j)[i][0], bounce(j, i), w_send.at[k, dst_core, j, i])

    def weight_write(k, dst_core, j, i):
        return pltpu.make_async_copy(bounce(j, i), weight_parts(k, dst_core, j)[i][1], w_recv.at[sy * lay_stage + k, j, i])

    def send_weights(k, part_lo, part_hi):
        parts = [(idx // 3 % 2, idx // 6, idx % 3) for idx in range(part_lo, part_hi)]
        for dst_core, j, i in parts:

            @pl.when(is_self(dst_core))
            def _():
                weight_read(k, dst_core, j, i).start()

            @pl.when(jnp.logical_not(is_self(dst_core)))
            def _():
                weight_remote(k, dst_core, j, i).start()

        for core in (0, 1):

            @pl.when(is_self(core))
            def _():
                for dst_core, j, i in parts:
                    if dst_core == core:
                        weight_read(k, dst_core, j, i).wait()
                        weight_write(k, dst_core, j, i).start()

    def finish_self(k):
        for core in (0, 1):

            @pl.when(is_self(core))
            def _():
                for j in range(2):
                    for i in range(3):
                        weight_write(k, core, j, i).wait()

    def landed(layer, j, i):
        dst = (w13_hbm.at[layer, j, :, pl.ds(0, ff)], w13_hbm.at[layer, j, :, pl.ds(ff, ff)], wd_hbm.at[layer, j])[i]
        src = (gate_hbm.at[0, 0], up_hbm.at[0, 0], down_hbm.at[0, 0])[i]
        return pltpu.make_async_copy(src, dst, w_recv.at[layer, j, i])

    def load_parts(layer, j):
        slot = layer % 2
        return (
            (w13_hbm.at[layer, j], w13_buf.at[slot, 2 * sc + j]),
            (wd_hbm.at[layer, j], wd_buf.at[slot, 2 * sc + j]),
        )

    def load_local(layer, j, i):
        src, dst = load_parts(layer, j)[i]
        return pltpu.make_async_copy(src, dst, load_sem.at[layer % 2, j, i])

    def load_push(layer, j, i):
        src, dst = load_parts(layer, j)[i]
        return pltpu.make_async_remote_copy(src, dst, push_send.at[layer % 2, j, i], push_recv.at[layer % 2, j, i], device_id=partner, device_id_type=MESH)

    def start_load(layer):
        @pl.when(layer >= 2)
        def _():
            pl.semaphore_wait(credit, 1)

        for j in range(2):
            @pl.when(jnp.logical_not((layer // lay_stage == sy) & (2 * sy + sx == sg)))
            def _():
                for i in range(3):
                    landed(layer, j, i).wait()

            for i in range(2):
                load_local(layer, j, i).start()
                load_push(layer, j, i).start()

    def finish_load(layer):
        for j in range(2):
            for i in range(2):
                load_local(layer, j, i).wait()
                load_push(layer, j, i).wait()

    def u_copy(t, h):
        src = u_buf.at[1 if t == 3 else 0, rows(h)]
        return pltpu.make_async_remote_copy(src, u_buf.at[t, rows(h)], u_send.at[t, h], u_recv.at[t, h], device_id=neighbour(h if t == 1 else 1 - h), device_id_type=MESH)

    def p_copy(t, h, q):
        return pltpu.make_async_remote_copy(p_buf.at[t, part(h, q)], r_buf.at[t, part(h, q)], p_send.at[t, h, q], p_recv.at[t, h, q], device_id=neighbour(1 - h if t == 2 else h), device_id_type=MESH)

    def g_copy(t, h):
        where = (1 - sy, 2 * (1 - sx) + sc) if t == 3 else neighbour(h if t == 1 else 1 - h)
        return pltpu.make_async_remote_copy(mix_vmem.at[rows(h)], g_buf.at[t, rows(h)], g_send.at[t, h], g_recv.at[t, h], device_id=where, device_id_type=MESH)

    def out_copy(layer):
        return pltpu.make_async_copy(h_buf.at[(layer + 1) % 2], hid_hbm.at[layer], out_sem.at[(layer + 1) % 2])

    halves = [(t, h) for t in (1, 2, 3) for h in (0, 1)]
    for t, h in halves:
        g_copy(t, h).start()
    send_weights(0, 0, 12)
    h_buf[0] = x_vmem[...].astype(jnp.float32)
    g_buf[0] = mix_vmem[...]
    for t, h in halves:
        g_copy(t, h).wait()

    lane = lax.broadcasted_iota(jnp.int32, g_buf.shape[1:], 1)

    @pl.loop(0, n_layers)
    def _(layer):
        slot = layer % 2
        h = h_buf[slot]
        u_buf[0] = (h * lax.rsqrt(jnp.mean(h * h, axis=-1, keepdims=True) + NORM_EPS)).astype(jnp.bfloat16)
        for t in (1, 2):
            for h in (0, 1):
                u_copy(t, h).start()

        @pl.when(layer < lay_stage)
        def _():
            finish_self(layer)
            start_load(layer)

        finish_load(layer)

        @pl.loop(0, 4)
        def _(b):
            @pl.when(b == 1)
            def _():
                for h in (0, 1):
                    u_copy(1, h).wait_recv()
                    u_copy(3, h).start()

            for t in (2, 3):

                @pl.when(b == t)
                def _():
                    for h in (0, 1):
                        u_copy(t, h).wait_recv()

            p_buf[b] = jnp.zeros(p_buf.shape[1:], jnp.float32)

            @pl.loop(0, exp_grp)
            def _(e):
                z = jnp.dot(u_buf[b], w13_buf[slot, e], preferred_element_type=jnp.float32)
                a = (jax.nn.silu(z[:, :ff]) * z[:, ff:]).astype(jnp.bfloat16)
                o = jnp.dot(a, wd_buf[slot, e], preferred_element_type=jnp.float32).astype(jnp.bfloat16).astype(jnp.float32)
                column = layer * n_experts + first_expert + e
                mix = jnp.sum(jnp.where(lane == column, g_buf[b], 0.0), axis=-1, keepdims=True)
                p_buf[b] = p_buf[b] + jnp.where(mix > 0.0, mix * o, 0.0)

            for t in (1, 3):

                @pl.when(b == t)
                def _():
                    for q in range(QUARTERS):
                        for h in (0, 1):
                            p_copy(t, h, q).start()

        @pl.when(layer < n_layers - 2)
        def _():
            pl.semaphore_signal(credit, 1, device_id=partner, device_id_type=MESH)

        @pl.when(layer < lay_stage - 1)
        def _():
            send_weights(layer + 1, 0, PART_A)

        for t, h in halves:
            u_copy(t, h).wait_send()
        for q in range(QUARTERS):
            for h in (0, 1):
                p_copy(3, h, q).wait_recv()
                p_buf[2, part(h, q)] = p_buf[2, part(h, q)] + r_buf[3, part(h, q)]
                p_copy(2, h, q).start()

        @pl.when(layer < lay_stage - 1)
        def _():
            send_weights(layer + 1, PART_A, 12)

        @pl.when((layer >= lay_stage - 1) & (layer < n_layers - 1))
        def _():
            start_load(layer + 1)

        @pl.when(layer >= 2)
        def _():
            out_copy(layer - 2).wait()

        for q in range(QUARTERS):
            for h in (0, 1):
                p_copy(3, h, q).wait_send()
                p_copy(1, h, q).wait()
        for q in range(QUARTERS):
            for h in (0, 1):
                p_copy(2, h, q).wait()
        h_buf[1 - slot] = h_buf[slot] + (p_buf[0] + r_buf[1] + r_buf[2])
        out_copy(layer).start()

    out_copy(n_layers - 2).wait()
    out_copy(n_layers - 1).wait()

    @pl.loop(0, lay_stage)
    def _(k):
        for idx in range(12):
            i, dst_core, j = idx % 3, (idx // 3) % 2, idx // 6

            @pl.when(jnp.logical_not(is_self(dst_core)))
            def _():
                weight_remote(k, dst_core, j, i).wait_send()


def place_kernel(w13_in, wd_in, hid_in, w13_out, wd_out, hid_out):
    w13_out[...] = w13_in[...]
    wd_out[...] = wd_in[...]
    hid_out[...] = hid_in[...]


def solution(mesh):
    n_stage = mesh.shape["stage"]
    n_group = mesh.shape["expert"]

    def per_device(gate_loc, up_loc, down_loc, x_loc, ids_loc, mix_loc):
        lay_stage, exp_grp, width, ff = gate_loc.shape
        n_layers, tok = ids_loc.shape[0], ids_loc.shape[1]
        n_experts = exp_grp * n_group
        exp_dev = exp_grp // n_stage
        onehot = ids_loc[..., None] == jnp.arange(n_experts, dtype=jnp.int32)
        dense = jnp.sum(jnp.where(onehot, mix_loc[..., None], 0.0), axis=2)
        dense = jnp.transpose(dense, (1, 0, 2)).reshape(tok, n_layers * n_experts)
        lanes = -(-dense.shape[1] // 128) * 128
        dense = jnp.pad(dense, ((0, 0), (0, lanes - dense.shape[1])))
        any_spec = pl.BlockSpec(memory_space=pl.ANY)
        vmem_spec = pl.BlockSpec(memory_space=pltpu.VMEM)
        dma = pltpu.SemaphoreType.DMA
        landed = pl.pallas_call(
            moe_kernel,
            out_shape=(
                jax.ShapeDtypeStruct((n_layers, exp_dev, width, 2 * ff), jnp.bfloat16),
                jax.ShapeDtypeStruct((n_layers, exp_dev, ff, width), jnp.bfloat16),
                jax.ShapeDtypeStruct((n_layers, tok, width), jnp.float32),
            ),
            in_specs=[any_spec, any_spec, any_spec, vmem_spec, vmem_spec],
            out_specs=(any_spec, any_spec, any_spec),
            scratch_shapes=[
                pltpu.VMEM((2, exp_grp, width, 2 * ff), jnp.bfloat16),
                pltpu.VMEM((2, exp_grp, ff, width), jnp.bfloat16),
                pltpu.VMEM((4, tok, width), jnp.bfloat16),
                pltpu.VMEM((4, tok, width), jnp.float32),
                pltpu.VMEM((4, tok, width), jnp.float32),
                pltpu.VMEM((2, tok, width), jnp.float32),
                pltpu.VMEM((4, tok, lanes), jnp.float32),
                pltpu.VMEM((exp_dev, width, 2 * ff), jnp.bfloat16),
                pltpu.VMEM((exp_dev, ff, width), jnp.bfloat16),
                dma((lay_stage, 2, 2, 3)),
                dma((n_layers, 2, 3)),
                dma((2, 2, 2)),
                dma((2, 2, 2)),
                dma((2, 2, 2)),
                dma((4, 2)),
                dma((4, 2)),
                dma((4, 2, QUARTERS)),
                dma((4, 2, QUARTERS)),
                dma((4, 2)),
                dma((4, 2)),
                dma((2,)),
                pltpu.SemaphoreType.REGULAR,
            ],
            compiler_params=pltpu.CompilerParams(has_side_effects=True, vmem_limit_bytes=60 * 1024 * 1024),
        )(gate_loc, up_loc, down_loc, x_loc, dense)
        blocks = [(1, 1, width, 2 * ff), (1, 1, ff, width)]
        specs = [pl.BlockSpec(block, lambda n: (n // exp_dev, n % exp_dev, 0, 0)) for block in blocks]
        specs.append(pl.BlockSpec((1, tok // exp_dev, width), lambda n: (n // exp_dev, n % exp_dev, 0)))
        return pl.pallas_call(
            place_kernel,
            out_shape=tuple(jax.ShapeDtypeStruct(one.shape, one.dtype) for one in landed),
            grid=(n_layers * exp_dev,),
            in_specs=specs,
            out_specs=tuple(specs),
            compiler_params=pltpu.CompilerParams(vmem_limit_bytes=60 * 1024 * 1024),
        )(*landed)

    weight_spec = P("stage", "expert")
    token_spec = P(None, FLAT)
    return jax.shard_map(per_device, mesh=mesh, in_specs=(weight_spec, weight_spec, weight_spec, P(FLAT), token_spec, token_spec), out_specs=(token_spec, token_spec, token_spec), check_vma=False)
```
